32 devices in a mesh: rep: 2 (over y), own: 16 (over z, x, core).
Axes of the slice: x: 2, y: 2, z: 4, core: 2. Of those that a mesh axis runs over, the one named last changes fastest.
Arguments:
- values: float32 [262144, 128], P(('rep', 'own')), may hold values from -0.8 to 0.8
- key_ids: int32 [262144], P(('rep', 'own')), may hold values from 0 to 65535, as said below
- heavy_ids: int32 [2048], replicated, may hold values from 0 to 65535, as said below
- block_offsets: int32 [32, 16], P(('rep', 'own')), may hold values from 0 to 8191, as said below
- block_counts: int32 [32, 16], P(('rep', 'own')), may hold values from 8 to 64, as said below
Outputs:
- light_sums: float32 [65536, 128], P('own')
- heavy_sums: float32 [2048, 128], P('own')
The draws below stay inside these ranges and needn't reach their ends.
Inputs may be any that keep to these rules, and one draw needn't show every extreme that they name: `key_ids`: an event in block o of a device has a key in o * 4096 to (o + 1) * 4096 - 1 that is not a heavy key; every event outside all blocks has a heavy key. `heavy_ids`: distinct keys. `block_offsets`: on each device the blocks lie in the order of o, do not meet, and end by position 8192. `block_counts`: at most 64; one owner gets exactly 64 from every device.
All inputs are finite; a program needn't handle non-finite values.
Results may differ from the reference program's by a relative error of at most 0.000075.
Values sent between devices are 32-bit elements; how exact they have to be, the bound alone decides.
A program may use at most 64 MiB of HBM per device.

```python
import jax
import jax.numpy as jnp

F = 128
H = 2048
KEYS_DEV = 4096
CAP = 64
EV_DEV = 8192
KEYS = 65536
EVENTS = 262144
N_REP = 2
N_OWN = 16


def layout_draw(key):
    devices = N_REP * N_OWN
    keys_all = KEYS_DEV * N_OWN
    shuffled = jax.random.permutation(jax.random.fold_in(key, 11), keys_all).astype(jnp.int32)
    heavy = shuffled[:H]
    flags = jnp.zeros((keys_all,), jnp.int32).at[heavy].set(1)
    per_owner = flags.reshape(N_OWN, KEYS_DEV)
    light_order = jnp.argsort(per_owner, axis=1, stable=True).astype(jnp.int32)
    light_count = (KEYS_DEV - jnp.sum(per_owner, axis=1)).astype(jnp.int32)
    lowest = CAP // 8
    owner_top = jax.random.randint(jax.random.fold_in(key, 12), (N_OWN,), CAP // 4, CAP + 1)
    counts = lowest + jax.random.randint(jax.random.fold_in(key, 13), (devices, N_OWN), 0, 1 << 20) % (owner_top - lowest + 1)[None, :]
    target = jax.random.randint(jax.random.fold_in(key, 14), (), 0, N_OWN)
    counts = counts.at[:, target].set(CAP)
    chosen = jax.random.randint(jax.random.fold_in(key, 15), (devices,), 0, N_OWN)
    counts = counts.at[jnp.arange(devices), chosen].set(CAP).astype(jnp.int32)
    spare = EV_DEV - jnp.sum(counts, axis=1)
    gaps = jax.random.randint(jax.random.fold_in(key, 16), (devices, N_OWN), 0, 1 << 20) % (spare[:, None] + 1)
    gaps = jnp.sort(gaps, axis=1)
    offsets = (jnp.cumsum(counts, axis=1) - counts + gaps).astype(jnp.int32)
    positions = jnp.arange(EV_DEV, dtype=jnp.int32)
    member = (positions[None, :, None] >= offsets[:, None, :]) & (positions[None, :, None] < (offsets + counts)[:, None, :])
    in_block = jnp.any(member, axis=2)
    owner = jnp.sum(member.astype(jnp.int32) * jnp.arange(N_OWN, dtype=jnp.int32)[None, None, :], axis=2)
    pick_light = jax.random.randint(jax.random.fold_in(key, 17), (devices, EV_DEV), 0, 1 << 20) % light_count[owner]
    light_key = owner * KEYS_DEV + light_order[owner, pick_light]
    first = jax.random.randint(jax.random.fold_in(key, 18), (devices, EV_DEV), 0, H)
    second = jax.random.randint(jax.random.fold_in(key, 19), (devices, EV_DEV), 0, H)
    third = jax.random.randint(jax.random.fold_in(key, 20), (devices, EV_DEV), 0, H)
    heavy_key = heavy[jnp.minimum(jnp.minimum(first, second), third)]
    key_ids = jnp.where(in_block, light_key, heavy_key).astype(jnp.int32).reshape(-1)
    return (key_ids, heavy, offsets, counts)


def draw_key_ids(key, part):
    return layout_draw(key)[0]


def draw_heavy_ids(key, part):
    return layout_draw(key)[1]


def draw_block_offsets(key, part):
    return layout_draw(key)[2]


def draw_block_counts(key, part):
    return layout_draw(key)[3]


def block_scale(stream_key, dims, cuts, low, high):
    level = 1.0
    for position, parts in cuts:
        steps = jax.random.uniform(jax.random.fold_in(jax.random.fold_in(stream_key, 6), position), (parts,), jnp.float32, low / len(cuts), high / len(cuts))
        level = level * jnp.repeat(jnp.exp(steps), dims[position] // parts).reshape((-1,) + (1,) * (len(dims) - 1 - position))
    return level


def normal_values(own_key, shape, deviation, reach, split=(), kind=jnp.bfloat16):
    factor_of = block_scale(own_key, shape, split, -0.22, 0.18) if split else 1.0
    drawn = jax.random.normal(own_key, shape, jnp.float32) * deviation * factor_of
    return jnp.minimum(jnp.maximum(drawn, -reach), reach).astype(kind)


def setup_inputs(seed: int = 0) -> dict:
    key_list = jax.random.split(jax.random.key(seed), 6)
    return {
        "values": normal_values(key_list[0], (EVENTS, F), 0.1, 0.8, ((0, 32),), jnp.float32),
        "key_ids": draw_key_ids(jax.random.fold_in(key_list[5], 71), 0),
        "heavy_ids": draw_heavy_ids(jax.random.fold_in(key_list[5], 71), 0),
        "block_offsets": draw_block_offsets(jax.random.fold_in(key_list[5], 71), 0),
        "block_counts": draw_block_counts(jax.random.fold_in(key_list[5], 71), 0),
    }


def reference(values, key_ids, heavy_ids, block_offsets, block_counts):
    positions = jnp.arange(EV_DEV, dtype=jnp.int32)
    starts = block_offsets[:, None, :]
    finish = (block_offsets + block_counts)[:, None, :]
    inside = jnp.any((positions[None, :, None] >= starts) & (positions[None, :, None] < finish), axis=2)
    inside = inside.reshape(-1)
    light_keys = jnp.where(inside, key_ids, KEYS).astype(jnp.int32)
    light_sums = jax.ops.segment_sum(values, light_keys, num_segments=KEYS + 1)[:KEYS]
    totals = jax.ops.segment_sum(values, key_ids, num_segments=KEYS)
    heavy_sums = totals[heavy_ids]
    return light_sums, heavy_sums
```

```python
import functools
import math

import jax
import jax.numpy as jnp
from jax import lax
from jax.experimental import pallas as pl
from jax.experimental.pallas import tpu as pltpu
from jax.sharding import PartitionSpec as P

CAP = 64
LANES = 128


def split_bf16(rows):
    high = rows.astype(jnp.bfloat16)
    low = (rows - high.astype(jnp.float32)).astype(jnp.bfloat16)
    return jnp.concatenate([high, low], axis=1)


def pack_kernel(owners, events, offs, cnts, vals, keys, out, stage, sems):
    def start_of(o):
        return jnp.minimum(offs[0, o], events - CAP)

    def copy_of(o):
        base = pl.multiple_of(jnp.minimum((start_of(o) // 8) * 8, events - CAP - 8), 8)
        return base, pltpu.make_async_copy(
            vals.at[pl.ds(base, CAP + 8)], stage.at[o], sems.at[o]
        )

    @pl.loop(0, owners)
    def _(o):
        copy_of(o)[1].start()

    lane = lax.broadcasted_iota(jnp.int32, (1, LANES), 1)
    last_row = events // LANES - 1

    @pl.loop(0, owners)
    def _(o):
        base, copy = copy_of(o)
        copy.wait()
        start = start_of(o)
        skip = offs[0, o] - start
        out[o, 0:CAP, :] = stage[o, pl.ds(start - base, CAP), :]
        row = start // LANES
        shift = start % LANES
        back = (LANES - shift) % LANES
        first = pltpu.roll(keys[pl.ds(row, 1), :], back, 1)
        second = pltpu.roll(keys[pl.ds(jnp.minimum(row + 1, last_row), 1), :], back, 1)
        joined = jnp.where(lane < LANES - shift, first, second)
        valid = (lane >= skip) & (lane < skip + cnts[0, o]) & (lane < CAP)
        block = jnp.where(valid, joined, -1)
        twice = jnp.where(lane < CAP, block, pltpu.roll(block, CAP, 1))
        out[o, CAP : CAP + 8, :] = jnp.broadcast_to(twice, (8, LANES)).astype(jnp.float32)


def pack(values, keys2d, offsets, counts, owners):
    events, width = values.shape
    smem = pl.BlockSpec(memory_space=pltpu.SMEM)
    vmem = pl.BlockSpec(memory_space=pltpu.VMEM)
    return pl.pallas_call(
        functools.partial(pack_kernel, owners, events),
        out_shape=jax.ShapeDtypeStruct((owners, CAP + 8, width), jnp.float32),
        in_specs=[smem, smem, pl.BlockSpec(memory_space=pl.ANY), vmem],
        out_specs=vmem,
        scratch_shapes=[
            pltpu.VMEM((owners, CAP + 8, width), jnp.float32),
            pltpu.SemaphoreType.DMA((owners,)),
        ],
        name="pack",
    )(offsets, counts, values, keys2d)


def heavy_kernel(step_k, pairs, rows_owner, vals, keys, heavy, out, rhs):
    events = vals.shape[0]
    steps = events // step_k
    chunk = heavy.shape[0]
    half = rows_owner // pairs

    @pl.when(pl.program_id(0) == 0)
    def _():
        @pl.loop(0, steps)
        def _(s):
            at = pl.ds(pl.multiple_of(s * step_k, step_k), step_k)
            rhs[at, :] = split_bf16(vals[at, :])

    targets = heavy[...]
    acc = jnp.zeros((chunk, rhs.shape[1]), jnp.float32)

    def body(s, acc):
        at = pl.ds(pl.multiple_of(s * step_k, step_k), step_k)
        pieces = []
        for c in range(step_k // LANES):
            row = keys[pl.ds(s * (step_k // LANES) + c, 1), :]
            pieces.append(jnp.where(targets == row, 1.0, 0.0).astype(jnp.bfloat16))
        onehot = jnp.concatenate(pieces, axis=1)
        return acc + jnp.dot(onehot, rhs[at, :], preferred_element_type=jnp.float32)

    acc = lax.fori_loop(0, steps, body, acc)
    width = vals.shape[1]
    sums = acc[:, :width] + acc[:, width:]
    for o in range(chunk // rows_owner):
        for r in range(pairs):
            begin = o * rows_owner + r * half
            out[r, o] = sums[begin : begin + half]


def heavy_partials(values, keys2d, heavy_wide, pairs, owners):
    events, width = values.shape
    heavy = heavy_wide.shape[0]
    rows_owner = heavy // owners
    chunk = max(rows_owner, min(256, heavy))
    per = chunk // rows_owner
    half = rows_owner // pairs
    return pl.pallas_call(
        functools.partial(heavy_kernel, 1024, pairs, rows_owner),
        out_shape=jax.ShapeDtypeStruct((pairs, owners, half, width), jnp.float32),
        grid=(heavy // chunk,),
        in_specs=[
            pl.BlockSpec((events, width), lambda i: (0, 0), pipeline_mode=pl.Buffered(1)),
            pl.BlockSpec(keys2d.shape, lambda i: (0, 0), pipeline_mode=pl.Buffered(1)),
            pl.BlockSpec((chunk, LANES), lambda i: (i, 0)),
        ],
        out_specs=pl.BlockSpec((pairs, per, half, width), lambda i: (0, i, 0, 0)),
        scratch_shapes=[pltpu.VMEM((events, 2 * width), jnp.bfloat16)],
        cost_estimate=pl.CostEstimate(
            flops=4 * heavy * events * width, bytes_accessed=4 * events * width, transcendentals=0
        ),
        compiler_params=pltpu.CompilerParams(dimension_semantics=("arbitrary",)),
        name="heavy",
    )(values, keys2d, heavy_wide)


def light_kernel(base_ref, got, out, rhs, rows):
    blocks = got.shape[0]
    width = got.shape[2]

    @pl.when(pl.program_id(0) == 0)
    def _():
        lane = lax.broadcasted_iota(jnp.int32, (1, LANES), 1)
        base = base_ref[0]

        @pl.loop(0, blocks // 2)
        def _(b):
            even = got[2 * b]
            odd = got[2 * b + 1]
            pair = jnp.concatenate([even[:CAP], odd[:CAP]], axis=0)
            rhs[pl.ds(pl.multiple_of(b * 2 * CAP, 2 * CAP), 2 * CAP), :] = split_bf16(pair)
            key = jnp.where(lane < CAP, even[CAP : CAP + 1], odd[CAP : CAP + 1])
            rows[pl.ds(b, 1), :] = key.astype(jnp.int32) - base

    tile = out.shape[0]
    mine = lax.broadcasted_iota(jnp.int32, (tile, LANES), 0) + pl.program_id(0) * tile
    acc = jnp.zeros((tile, 2 * width), jnp.float32)
    per = math.gcd(8, blocks // 2)
    step_k = per * LANES

    def body(s, acc):
        pieces = []
        for c in range(per):
            row = rows[pl.ds(s * per + c, 1), :]
            pieces.append(jnp.where(mine == row, 1.0, 0.0).astype(jnp.bfloat16))
        onehot = jnp.concatenate(pieces, axis=1)
        at = pl.ds(pl.multiple_of(s * step_k, step_k), step_k)
        return acc + jnp.dot(onehot, rhs[at, :], preferred_element_type=jnp.float32)

    acc = lax.fori_loop(0, blocks * CAP // step_k, body, acc)
    out[...] = acc[:, :width] + acc[:, width:]


def light_totals(got, base, keys_dev):
    blocks, unused, width = got.shape
    tile = 256
    return pl.pallas_call(
        light_kernel,
        out_shape=jax.ShapeDtypeStruct((keys_dev, width), jnp.float32),
        grid=(keys_dev // tile,),
        in_specs=[
            pl.BlockSpec(memory_space=pltpu.SMEM),
            pl.BlockSpec(got.shape, lambda i: (0, 0, 0), pipeline_mode=pl.Buffered(1)),
        ],
        out_specs=pl.BlockSpec((tile, width), lambda i: (i, 0)),
        scratch_shapes=[
            pltpu.VMEM((blocks * CAP, 2 * width), jnp.bfloat16),
            pltpu.VMEM((blocks // 2, LANES), jnp.int32),
        ],
        cost_estimate=pl.CostEstimate(
            flops=4 * keys_dev * blocks * CAP * width,
            bytes_accessed=4 * keys_dev * width,
            transcendentals=0,
        ),
        compiler_params=pltpu.CompilerParams(dimension_semantics=("arbitrary",)),
        name="light",
    )(base, got)


KEYS_DEV = 4096


def per_device(values, key_ids, heavy_ids, block_offsets, block_counts):
    owners = lax.axis_size("own")
    pairs = lax.axis_size("rep")
    own_index = lax.axis_index("own")
    events, width = values.shape
    keys2d = key_ids.reshape(events // LANES, LANES)
    payload = pack(values, keys2d, block_offsets, block_counts, owners)
    payload = jnp.concatenate([payload] * pairs, axis=0)
    got = lax.all_to_all(payload, ("rep", "own"), split_axis=0, concat_axis=0, tiled=True)
    heavy_wide = jnp.broadcast_to(heavy_ids[:, None], (heavy_ids.shape[0], LANES))
    partial = heavy_partials(values, keys2d, heavy_wide, pairs, owners)
    partial = partial.reshape((pairs * owners,) + partial.shape[2:])
    swapped = lax.all_to_all(partial, ("rep", "own"), split_axis=0, concat_axis=0, tiled=True)
    base = (own_index * KEYS_DEV).astype(jnp.int32).reshape(1)
    light_sums = light_totals(got, base, KEYS_DEV)
    mine = jnp.sum(swapped, axis=0)
    heavy_sums = lax.all_gather(mine, "rep", axis=0, tiled=True)
    return (light_sums, heavy_sums)


def solution(mesh):
    placed = (
        P(("rep", "own"), None),
        P(("rep", "own")),
        P(),
        P(("rep", "own"), None),
        P(("rep", "own"), None),
    )
    return jax.shard_map(
        per_device,
        mesh=mesh,
        in_specs=placed,
        out_specs=(P("own", None), P("own", None)),
        check_vma=False,
    )
```

```python
import functools
import math

import jax
import jax.numpy as jnp
from jax import lax
from jax.experimental import pallas as pl
from jax.experimental.pallas import tpu as pltpu
from jax.sharding import PartitionSpec as P

CAP = 64
LANES = 128
MESH = pl.DeviceIdType.MESH


def split_bf16(rows):
    high = rows.astype(jnp.bfloat16)
    low = (rows - high.astype(jnp.float32)).astype(jnp.bfloat16)
    return jnp.concatenate([high, low], axis=1)


def pack_kernel(owners, events, offs, cnts, vals, keys, out, stage, sems):
    def start_of(o):
        return jnp.minimum(offs[0, o], events - CAP)

    def copy_of(o):
        base = pl.multiple_of(jnp.minimum((start_of(o) // 8) * 8, events - CAP - 8), 8)
        return base, pltpu.make_async_copy(
            vals.at[pl.ds(base, CAP + 8)], stage.at[o], sems.at[o]
        )

    @pl.loop(0, owners)
    def _(o):
        copy_of(o)[1].start()

    lane = lax.broadcasted_iota(jnp.int32, (1, LANES), 1)
    last_row = events // LANES - 1

    @pl.loop(0, owners)
    def _(o):
        base, copy = copy_of(o)
        copy.wait()
        start = start_of(o)
        skip = offs[0, o] - start
        out[o, 0:CAP, :] = stage[o, pl.ds(start - base, CAP), :]
        row = start // LANES
        shift = start % LANES
        back = (LANES - shift) % LANES
        first = pltpu.roll(keys[pl.ds(row, 1), :], back, 1)
        second = pltpu.roll(keys[pl.ds(jnp.minimum(row + 1, last_row), 1), :], back, 1)
        joined = jnp.where(lane < LANES - shift, first, second)
        valid = (lane >= skip) & (lane < skip + cnts[0, o]) & (lane < CAP)
        block = jnp.where(valid, joined, -1)
        twice = jnp.where(lane < CAP, block, pltpu.roll(block, CAP, 1))
        out[o, CAP : CAP + 8, :] = jnp.broadcast_to(twice, (8, LANES)).astype(jnp.float32)


def pack(values, keys2d, offsets, counts, owners):
    events, width = values.shape
    smem = pl.BlockSpec(memory_space=pltpu.SMEM)
    vmem = pl.BlockSpec(memory_space=pltpu.VMEM)
    return pl.pallas_call(
        functools.partial(pack_kernel, owners, events),
        out_shape=jax.ShapeDtypeStruct((owners, CAP + 8, width), jnp.float32),
        in_specs=[smem, smem, pl.BlockSpec(memory_space=pl.ANY), vmem],
        out_specs=vmem,
        scratch_shapes=[
            pltpu.VMEM((owners, CAP + 8, width), jnp.float32),
            pltpu.SemaphoreType.DMA((owners,)),
        ],
        name="pack",
    )(offsets, counts, values, keys2d)


def exchange_kernel(
    pairs, owners, step_k, payload, vals, keys, heavy, got, sums_out,
    staged, rhs, part, quad, mine, landed, final,
    vs, ls, lr, fs, fr, qs, qr, ts, tr, es, er,
):
    r = lax.axis_index("rep")
    own = lax.axis_index("own")
    core = lax.rem(own, 2)
    chip = lax.div(own, 2)
    chips = owners // 2
    events, width = vals.shape
    steps = events // step_k
    chunk = heavy.shape[0] // chips
    rows_owner = chunk // 2
    half = rows_owner // pairs
    members = 2 * pairs

    def value_copy(s):
        at = pl.ds(pl.multiple_of(s * step_k, step_k), step_k)
        return pltpu.make_async_copy(vals.at[at], staged.at[at], vs.at[s])

    for s in range(steps):
        value_copy(s).start()

    barrier = pltpu.get_barrier_semaphore()

    @pl.loop(1, owners)
    def _(d):
        pl.semaphore_signal(
            barrier, 1, device_id=(r, lax.rem(own + d, owners)), device_id_type=MESH
        )

    for m in range(2, members):
        pl.semaphore_signal(
            barrier, 1,
            device_id=(lax.rem(r + m // 2, pairs), 2 * chip + lax.rem(core + m, 2)),
            device_id_type=MESH,
        )
    pl.semaphore_wait(barrier, owners - 1 + members - 2)

    def light(d):
        dest = lax.rem(own + d, owners)
        return pltpu.make_async_remote_copy(
            src_ref=payload.at[dest], dst_ref=got.at[r * owners + own],
            send_sem=ls.at[d], recv_sem=lr.at[d],
            device_id=(r, dest), device_id_type=MESH,
        )

    here = pltpu.make_async_copy(payload.at[own], got.at[r * owners + own], ls.at[0])
    here.start()

    @pl.loop(1, owners)
    def _(d):
        light(d).start()

    def forward(d, q):
        slot = r * owners + lax.rem(own - d + owners, owners)
        return pltpu.make_async_remote_copy(
            src_ref=got.at[slot], dst_ref=got.at[slot],
            send_sem=fs.at[q - 1, d], recv_sem=fr.at[q - 1, d],
            device_id=(lax.rem(r + q, pairs), own), device_id_type=MESH,
        )

    def gather_quad(c, m):
        peer_r = lax.rem(r + m // 2, pairs)
        peer_k = lax.rem(core + m, 2)
        return pltpu.make_async_remote_copy(
            src_ref=part.at[c, peer_r, peer_k], dst_ref=quad.at[c, m - 1],
            send_sem=qs.at[c, m - 1], recv_sem=qr.at[c, m - 1],
            device_id=(peer_r, 2 * chip + peer_k), device_id_type=MESH,
        )

    def deliver(c):
        return pltpu.make_async_remote_copy(
            src_ref=mine.at[c], dst_ref=landed.at[chip],
            send_sem=ts.at[c], recv_sem=tr.at[chip],
            device_id=(r, 2 * c + core), device_id_type=MESH,
        )

    def arrival(c):
        return pltpu.make_async_remote_copy(
            src_ref=mine.at[c], dst_ref=landed.at[c],
            send_sem=ts.at[c], recv_sem=tr.at[c],
            device_id=(r, 2 * c + core), device_id_type=MESH,
        )

    for s in range(steps):
        value_copy(s).wait()
        rhs[s * step_k : (s + 1) * step_k, :] = split_bf16(staged[s * step_k : (s + 1) * step_k, :])

    group = owners // (chips // 2)
    first_forward = chips - chips // 2

    def chunk_at(i):
        return lax.rem(chip + 1 + i, chips)

    @pl.loop(0, chips + 4)
    def _(i):
        @pl.when(i < chips)
        def _():
            c = chunk_at(i)
            targets = heavy[pl.ds(pl.multiple_of(c * chunk, chunk), chunk), :]

            def body(s, acc):
                at = pl.ds(pl.multiple_of(s * step_k, step_k), step_k)
                pieces = []
                for p in range(step_k // LANES):
                    row = keys[pl.ds(s * (step_k // LANES) + p, 1), :]
                    pieces.append(jnp.where(targets == row, 1.0, 0.0).astype(jnp.bfloat16))
                onehot = jnp.concatenate(pieces, axis=1)
                return acc + jnp.dot(onehot, rhs[at, :], preferred_element_type=jnp.float32)

            acc = lax.fori_loop(0, steps, body, jnp.zeros((chunk, 2 * width), jnp.float32))
            sums = acc[:, :width] + acc[:, width:]
            for k in range(2):
                for side in range(pairs):
                    begin = k * rows_owner + side * half
                    part[c, side, k] = sums[begin : begin + half]

        @pl.when((i >= 1) & (i < chips + 1))
        def _():
            c = chunk_at(i - 1)
            for m in range(1, members):
                gather_quad(c, m).start()

        @pl.when((i >= first_forward) & (i < chips))
        def _():
            for g in range(group):
                d = (i - first_forward) * group + g

                @pl.when(d == 0)
                def _():
                    here.wait()

                @pl.when(d > 0)
                def _():
                    light(d).wait_recv()

                for q in range(1, pairs):
                    forward(d, q).start()

        @pl.when((i >= 4) & (i < chips + 4))
        def _():
            c = chunk_at(i - 4)

            @pl.when(c != chip)
            def _():
                deliver(c).start()

        @pl.when((i >= 3) & (i < chips + 3))
        def _():
            c = chunk_at(i - 3)
            total = part[c, r, core]
            for m in range(1, members):
                gather_quad(c, m).wait_recv()
                total = total + quad[c, m - 1]
            mine[c] = total

    total = mine[chip]
    for j in range(1, chips):
        c = lax.rem(chip + chips - j, chips)
        arrival(c).wait_recv()
        total = total + landed[c]
    final[r] = total

    @pl.loop(0, owners)
    def _(d):
        for q in range(1, pairs):
            forward(d, q).wait_recv()

        @pl.when(d > 0)
        def _():
            light(d).wait_send()

    def share(q):
        return pltpu.make_async_remote_copy(
            src_ref=final.at[r], dst_ref=final.at[r],
            send_sem=es.at[q - 1], recv_sem=er.at[q - 1],
            device_id=(lax.rem(r + q, pairs), own), device_id_type=MESH,
        )

    for q in range(1, pairs):
        share(q).start()

    @pl.loop(0, owners)
    def _(d):
        for q in range(1, pairs):
            forward(d, q).wait_send()

    @pl.loop(0, chips)
    def _(c):
        for m in range(1, members):
            gather_quad(c, m).wait_send()

        @pl.when(c != chip)
        def _():
            deliver(c).wait_send()

    for q in range(1, pairs):
        back = lax.rem(r - q + pairs, pairs)
        pltpu.make_async_remote_copy(
            src_ref=final.at[back], dst_ref=final.at[back],
            send_sem=es.at[q - 1], recv_sem=er.at[q - 1],
            device_id=(lax.rem(r + q, pairs), own), device_id_type=MESH,
        ).wait_recv()
        share(q).wait_send()
    for side in range(pairs):
        sums_out[side * half : (side + 1) * half, :] = final[side]


def exchange(payload, values, keys2d, heavy_wide, pairs, owners):
    events, width = values.shape
    heavy = heavy_wide.shape[0]
    rows_owner = heavy // owners
    half = rows_owner // pairs
    chips = owners // 2
    step_k = 1024
    vmem = pl.BlockSpec(memory_space=pltpu.VMEM)
    dma = pltpu.SemaphoreType.DMA
    members = 2 * pairs
    return pl.pallas_call(
        functools.partial(exchange_kernel, pairs, owners, step_k),
        out_shape=(
            jax.ShapeDtypeStruct((pairs * owners, CAP + 8, width), jnp.float32),
            jax.ShapeDtypeStruct((rows_owner, width), jnp.float32),
        ),
        in_specs=[vmem, pl.BlockSpec(memory_space=pl.ANY), vmem, vmem],
        out_specs=(vmem, vmem),
        scratch_shapes=[
            pltpu.VMEM((events, width), jnp.float32),
            pltpu.VMEM((events, 2 * width), jnp.bfloat16),
            pltpu.VMEM((chips, pairs, 2, half, width), jnp.float32),
            pltpu.VMEM((chips, members - 1, half, width), jnp.float32),
            pltpu.VMEM((chips, half, width), jnp.float32),
            pltpu.VMEM((chips, half, width), jnp.float32),
            pltpu.VMEM((pairs, half, width), jnp.float32),
            dma((events // step_k,)),
            dma((owners,)),
            dma((owners,)),
            dma((pairs - 1, owners)),
            dma((pairs - 1, owners)),
            dma((chips, members - 1)),
            dma((chips, members - 1)),
            dma((chips,)),
            dma((chips,)),
            dma((pairs - 1,)),
            dma((pairs - 1,)),
        ],
        cost_estimate=pl.CostEstimate(
            flops=4 * heavy * events * width, bytes_accessed=4 * events * width, transcendentals=0
        ),
        compiler_params=pltpu.CompilerParams(
            collective_id=0, has_side_effects=True, vmem_limit_bytes=50 * 1024 * 1024
        ),
        name="exchange",
    )(payload, values, keys2d, heavy_wide)


def light_kernel(base_ref, got, out, rhs, rows):
    blocks = got.shape[0]
    width = got.shape[2]

    @pl.when(pl.program_id(0) == 0)
    def _():
        lane = lax.broadcasted_iota(jnp.int32, (1, LANES), 1)
        base = base_ref[0]

        @pl.loop(0, blocks // 2)
        def _(b):
            even = got[2 * b]
            odd = got[2 * b + 1]
            pair = jnp.concatenate([even[:CAP], odd[:CAP]], axis=0)
            rhs[pl.ds(pl.multiple_of(b * 2 * CAP, 2 * CAP), 2 * CAP), :] = split_bf16(pair)
            key = jnp.where(lane < CAP, even[CAP : CAP + 1], odd[CAP : CAP + 1])
            rows[pl.ds(b, 1), :] = key.astype(jnp.int32) - base

    tile = out.shape[0]
    mine = lax.broadcasted_iota(jnp.int32, (tile, LANES), 0) + pl.program_id(0) * tile
    acc = jnp.zeros((tile, 2 * width), jnp.float32)
    per = math.gcd(8, blocks // 2)
    step_k = per * LANES

    def body(s, acc):
        pieces = []
        for c in range(per):
            row = rows[pl.ds(s * per + c, 1), :]
            pieces.append(jnp.where(mine == row, 1.0, 0.0).astype(jnp.bfloat16))
        onehot = jnp.concatenate(pieces, axis=1)
        at = pl.ds(pl.multiple_of(s * step_k, step_k), step_k)
        return acc + jnp.dot(onehot, rhs[at, :], preferred_element_type=jnp.float32)

    acc = lax.fori_loop(0, blocks * CAP // step_k, body, acc)
    out[...] = acc[:, :width] + acc[:, width:]


def light_totals(got, base, keys_dev):
    blocks, unused, width = got.shape
    tile = 256
    return pl.pallas_call(
        light_kernel,
        out_shape=jax.ShapeDtypeStruct((keys_dev, width), jnp.float32),
        grid=(keys_dev // tile,),
        in_specs=[
            pl.BlockSpec(memory_space=pltpu.SMEM),
            pl.BlockSpec(got.shape, lambda i: (0, 0, 0), pipeline_mode=pl.Buffered(1)),
        ],
        out_specs=pl.BlockSpec((tile, width), lambda i: (i, 0)),
        scratch_shapes=[
            pltpu.VMEM((blocks * CAP, 2 * width), jnp.bfloat16),
            pltpu.VMEM((blocks // 2, LANES), jnp.int32),
        ],
        cost_estimate=pl.CostEstimate(
            flops=4 * keys_dev * blocks * CAP * width,
            bytes_accessed=4 * keys_dev * width,
            transcendentals=0,
        ),
        compiler_params=pltpu.CompilerParams(dimension_semantics=("arbitrary",)),
        name="light",
    )(base, got)


KEYS_DEV = 4096


def per_device(values, key_ids, heavy_ids, block_offsets, block_counts):
    owners = lax.axis_size("own")
    pairs = lax.axis_size("rep")
    own_index = lax.axis_index("own")
    events, width = values.shape
    keys2d = key_ids.reshape(events // LANES, LANES)
    payload = pack(values, keys2d, block_offsets, block_counts, owners)
    heavy_wide = jnp.broadcast_to(heavy_ids[:, None], (heavy_ids.shape[0], LANES))
    got, heavy_sums = exchange(payload, values, keys2d, heavy_wide, pairs, owners)
    base = (own_index * KEYS_DEV).astype(jnp.int32).reshape(1)
    light_sums = light_totals(got, base, KEYS_DEV)
    return (light_sums, heavy_sums)


def solution(mesh):
    placed = (
        P(("rep", "own"), None),
        P(("rep", "own")),
        P(),
        P(("rep", "own"), None),
        P(("rep", "own"), None),
    )
    return jax.shard_map(
        per_device,
        mesh=mesh,
        in_specs=placed,
        out_specs=(P("own", None), P("own", None)),
        check_vma=False,
    )
```

```python
import functools
import math

import jax
import jax.numpy as jnp
from jax import lax
from jax.experimental import pallas as pl
from jax.experimental.pallas import tpu as pltpu
from jax.sharding import PartitionSpec as P

CAP = 64
LANES = 128
MESH = pl.DeviceIdType.MESH


def split_bf16(rows):
    high = rows.astype(jnp.bfloat16)
    low = (rows - high.astype(jnp.float32)).astype(jnp.bfloat16)
    return jnp.concatenate([high, low], axis=1)


def pack_kernel(owners, events, offs, cnts, vals, keys, out, stage, sems):
    def start_of(o):
        return jnp.minimum(offs[0, o], events - CAP)

    def base_of(o):
        return pl.multiple_of(jnp.minimum((start_of(o) // 8) * 8, events - CAP - 8), 8)

    def copy_of(o):
        return pltpu.make_async_copy(
            vals.at[pl.ds(base_of(o), CAP + 8)], stage.at[o], sems.at[o]
        )

    @pl.loop(0, owners)
    def _(o):
        copy_of(o).start()

    lane = lax.broadcasted_iota(jnp.int32, (1, LANES), 1)
    last_row = events // LANES - 1

    @pl.loop(0, owners)
    def _(o):
        copy_of(o).wait()

    def fill(o):
        base = base_of(o)
        start = start_of(o)
        skip = offs[0, o] - start
        out[o, 0:CAP, :] = stage[o, pl.ds(start - base, CAP), :]
        row = start // LANES
        shift = start % LANES
        back = (LANES - shift) % LANES
        first = pltpu.roll(keys[pl.ds(row, 1), :], back, 1)
        second = pltpu.roll(keys[pl.ds(jnp.minimum(row + 1, last_row), 1), :], back, 1)
        joined = jnp.where(lane < LANES - shift, first, second)
        valid = (lane >= skip) & (lane < skip + cnts[0, o]) & (lane < CAP)
        block = jnp.where(valid, joined, -1)
        twice = jnp.where(lane < CAP, block, pltpu.roll(block, CAP, 1))
        out[o, CAP : CAP + 8, :] = jnp.broadcast_to(twice, (8, LANES)).astype(jnp.float32)

    unroll = math.gcd(owners, 8)

    @pl.loop(0, owners // unroll)
    def _(g):
        for u in range(unroll):
            fill(g * unroll + u)


def pack(values, keys2d, offsets, counts, owners):
    events, width = values.shape
    smem = pl.BlockSpec(memory_space=pltpu.SMEM)
    vmem = pl.BlockSpec(memory_space=pltpu.VMEM)
    return pl.pallas_call(
        functools.partial(pack_kernel, owners, events),
        out_shape=jax.ShapeDtypeStruct((owners, CAP + 8, width), jnp.float32),
        in_specs=[smem, smem, pl.BlockSpec(memory_space=pl.ANY), vmem],
        out_specs=vmem,
        scratch_shapes=[
            pltpu.VMEM((owners, CAP + 8, width), jnp.float32),
            pltpu.SemaphoreType.DMA((owners,)),
        ],
        name="pack",
    )(offsets, counts, values, keys2d)


def exchange_kernel(
    pairs, owners, step_k, payload, vals, keys, heavy, got, sums_out,
    staged, rhs, part, quad, mine, landed, final,
    vs, ls, lr, fs, fr, qs, qr, ts, tr, es, er,
):
    r = lax.axis_index("rep")
    own = lax.axis_index("own")
    core = lax.rem(own, 2)
    chip = lax.div(own, 2)
    chips = owners // 2
    events, width = vals.shape
    steps = events // step_k
    chunk = heavy.shape[0] // chips
    rows_owner = chunk // 2
    half = rows_owner // pairs
    members = 2 * pairs

    def value_copy(s):
        at = pl.ds(pl.multiple_of(s * step_k, step_k), step_k)
        return pltpu.make_async_copy(vals.at[at], staged.at[at], vs.at[s])

    for s in range(steps):
        value_copy(s).start()

    barrier = pltpu.get_barrier_semaphore()

    @pl.loop(1, owners)
    def _(d):
        pl.semaphore_signal(
            barrier, 1, device_id=(r, lax.rem(own + d, owners)), device_id_type=MESH
        )

    for m in range(2, members):
        pl.semaphore_signal(
            barrier, 1,
            device_id=(lax.rem(r + m // 2, pairs), 2 * chip + lax.rem(core + m, 2)),
            device_id_type=MESH,
        )
    pl.semaphore_wait(barrier, owners - 1 + members - 2)

    def light(d):
        dest = lax.rem(own + d, owners)
        return pltpu.make_async_remote_copy(
            src_ref=payload.at[dest], dst_ref=got.at[r * owners + own],
            send_sem=ls.at[d], recv_sem=lr.at[d],
            device_id=(r, dest), device_id_type=MESH,
        )

    here = pltpu.make_async_copy(payload.at[own], got.at[r * owners + own], ls.at[0])
    here.start()

    @pl.loop(1, owners)
    def _(d):
        light(d).start()

    def forward(d, q):
        slot = r * owners + lax.rem(own - d + owners, owners)
        return pltpu.make_async_remote_copy(
            src_ref=got.at[slot], dst_ref=got.at[slot],
            send_sem=fs.at[q - 1, d], recv_sem=fr.at[q - 1, d],
            device_id=(lax.rem(r + q, pairs), own), device_id_type=MESH,
        )

    def gather_quad(c, m):
        peer_r = lax.rem(r + m // 2, pairs)
        peer_k = lax.rem(core + m, 2)
        return pltpu.make_async_remote_copy(
            src_ref=part.at[c, peer_r, peer_k], dst_ref=quad.at[c, m - 1],
            send_sem=qs.at[c, m - 1], recv_sem=qr.at[c, m - 1],
            device_id=(peer_r, 2 * chip + peer_k), device_id_type=MESH,
        )

    def deliver(c):
        return pltpu.make_async_remote_copy(
            src_ref=mine.at[c], dst_ref=landed.at[chip],
            send_sem=ts.at[c], recv_sem=tr.at[chip],
            device_id=(r, 2 * c + core), device_id_type=MESH,
        )

    def arrival(c):
        return pltpu.make_async_remote_copy(
            src_ref=mine.at[c], dst_ref=landed.at[c],
            send_sem=ts.at[c], recv_sem=tr.at[c],
            device_id=(r, 2 * c + core), device_id_type=MESH,
        )

    for s in range(steps):
        value_copy(s).wait()
        rhs[s * step_k : (s + 1) * step_k, :] = split_bf16(staged[s * step_k : (s + 1) * step_k, :])

    group = owners // chips
    first_forward = min(3, chips)

    def chunk_at(i):
        return lax.rem(chip + 1 + i, chips)

    @pl.loop(0, chips + 4)
    def _(i):
        @pl.when(i < chips)
        def _():
            c = chunk_at(i)
            targets = heavy[pl.ds(pl.multiple_of(c * chunk, chunk), chunk), :]

            pieces = []
            for p in range(events // LANES):
                row = keys[p : p + 1, :]
                pieces.append(jnp.where(targets == row, 1.0, 0.0).astype(jnp.bfloat16))
            onehot = jnp.concatenate(pieces, axis=1)
            acc = jnp.dot(onehot, rhs[...], preferred_element_type=jnp.float32)
            sums = acc[:, :width] + acc[:, width:]
            for k in range(2):
                for side in range(pairs):
                    begin = k * rows_owner + side * half
                    part[c, side, k] = sums[begin : begin + half]

        @pl.when((i >= 1) & (i < chips + 1))
        def _():
            c = chunk_at(i - 1)
            for m in range(1, members):
                gather_quad(c, m).start()

        @pl.when((i >= 4) & (i < chips + 4))
        def _():
            c = chunk_at(i - 4)

            @pl.when(c != chip)
            def _():
                deliver(c).start()

        @pl.when((i >= 3) & (i < chips + 3))
        def _():
            c = chunk_at(i - 3)
            total = part[c, r, core]
            for m in range(1, members):
                gather_quad(c, m).wait_recv()
                total = total + quad[c, m - 1]
            mine[c] = total

        @pl.when((i >= first_forward) & (i < first_forward + chips))
        def _():
            for g in range(group):
                d = (i - first_forward) * group + g

                @pl.when(d == 0)
                def _():
                    here.wait()

                @pl.when(d > 0)
                def _():
                    light(d).wait_recv()

                for q in range(1, pairs):
                    forward(d, q).start()

    total = mine[chip]
    for j in range(1, chips):
        c = lax.rem(chip + chips - j, chips)
        arrival(c).wait_recv()
        total = total + landed[c]
    final[r] = total

    @pl.loop(0, owners)
    def _(d):
        for q in range(1, pairs):
            forward(d, q).wait_recv()

        @pl.when(d > 0)
        def _():
            light(d).wait_send()

    def share(q):
        return pltpu.make_async_remote_copy(
            src_ref=final.at[r], dst_ref=final.at[r],
            send_sem=es.at[q - 1], recv_sem=er.at[q - 1],
            device_id=(lax.rem(r + q, pairs), own), device_id_type=MESH,
        )

    for q in range(1, pairs):
        share(q).start()

    @pl.loop(0, owners)
    def _(d):
        for q in range(1, pairs):
            forward(d, q).wait_send()

    @pl.loop(0, chips)
    def _(c):
        for m in range(1, members):
            gather_quad(c, m).wait_send()

        @pl.when(c != chip)
        def _():
            deliver(c).wait_send()

    for q in range(1, pairs):
        back = lax.rem(r - q + pairs, pairs)
        pltpu.make_async_remote_copy(
            src_ref=final.at[back], dst_ref=final.at[back],
            send_sem=es.at[q - 1], recv_sem=er.at[q - 1],
            device_id=(lax.rem(r + q, pairs), own), device_id_type=MESH,
        ).wait_recv()
        share(q).wait_send()
    for side in range(pairs):
        sums_out[side * half : (side + 1) * half, :] = final[side]


def exchange(payload, values, keys2d, heavy_wide, pairs, owners):
    events, width = values.shape
    heavy = heavy_wide.shape[0]
    rows_owner = heavy // owners
    half = rows_owner // pairs
    chips = owners // 2
    step_k = 1024
    vmem = pl.BlockSpec(memory_space=pltpu.VMEM)
    dma = pltpu.SemaphoreType.DMA
    members = 2 * pairs
    return pl.pallas_call(
        functools.partial(exchange_kernel, pairs, owners, step_k),
        out_shape=(
            jax.ShapeDtypeStruct((pairs * owners, CAP + 8, width), jnp.float32),
            jax.ShapeDtypeStruct((rows_owner, width), jnp.float32),
        ),
        in_specs=[vmem, pl.BlockSpec(memory_space=pl.ANY), vmem, vmem],
        out_specs=(vmem, vmem),
        scratch_shapes=[
            pltpu.VMEM((events, width), jnp.float32),
            pltpu.VMEM((events, 2 * width), jnp.bfloat16),
            pltpu.VMEM((chips, pairs, 2, half, width), jnp.float32),
            pltpu.VMEM((chips, members - 1, half, width), jnp.float32),
            pltpu.VMEM((chips, half, width), jnp.float32),
            pltpu.VMEM((chips, half, width), jnp.float32),
            pltpu.VMEM((pairs, half, width), jnp.float32),
            dma((events // step_k,)),
            dma((owners,)),
            dma((owners,)),
            dma((pairs - 1, owners)),
            dma((pairs - 1, owners)),
            dma((chips, members - 1)),
            dma((chips, members - 1)),
            dma((chips,)),
            dma((chips,)),
            dma((pairs - 1,)),
            dma((pairs - 1,)),
        ],
        cost_estimate=pl.CostEstimate(
            flops=4 * heavy * events * width, bytes_accessed=4 * events * width, transcendentals=0
        ),
        compiler_params=pltpu.CompilerParams(
            collective_id=0, has_side_effects=True, vmem_limit_bytes=50 * 1024 * 1024
        ),
        name="exchange",
    )(payload, values, keys2d, heavy_wide)


def light_kernel(base_ref, got, out, rhs, rows):
    blocks = got.shape[0]
    width = got.shape[2]

    @pl.when(pl.program_id(0) == 0)
    def _():
        lane = lax.broadcasted_iota(jnp.int32, (1, LANES), 1)
        base = base_ref[0]

        def stage(b):
            even = got[2 * b]
            odd = got[2 * b + 1]
            pair = jnp.concatenate([even[:CAP], odd[:CAP]], axis=0)
            rhs[pl.ds(pl.multiple_of(b * 2 * CAP, 2 * CAP), 2 * CAP), :] = split_bf16(pair)
            key = jnp.where(lane < CAP, even[CAP : CAP + 1], odd[CAP : CAP + 1])
            rows[pl.ds(b, 1), :] = key.astype(jnp.int32) - base

        unroll = math.gcd(blocks // 2, 4)

        @pl.loop(0, blocks // 2 // unroll)
        def _(g):
            for u in range(unroll):
                stage(g * unroll + u)

    tile = out.shape[0]
    mine = lax.broadcasted_iota(jnp.int32, (tile, LANES), 0) + pl.program_id(0) * tile
    pieces = []
    for c in range(blocks // 2):
        row = rows[c : c + 1, :]
        pieces.append(jnp.where(mine == row, 1.0, 0.0).astype(jnp.bfloat16))
    onehot = jnp.concatenate(pieces, axis=1)
    acc = jnp.dot(onehot, rhs[...], preferred_element_type=jnp.float32)
    out[...] = acc[:, :width] + acc[:, width:]


def light_totals(got, base, keys_dev):
    blocks, unused, width = got.shape
    tile = math.gcd(keys_dev, 512)
    return pl.pallas_call(
        light_kernel,
        out_shape=jax.ShapeDtypeStruct((keys_dev, width), jnp.float32),
        grid=(keys_dev // tile,),
        in_specs=[
            pl.BlockSpec(memory_space=pltpu.SMEM),
            pl.BlockSpec(got.shape, lambda i: (0, 0, 0), pipeline_mode=pl.Buffered(1)),
        ],
        out_specs=pl.BlockSpec((tile, width), lambda i: (i, 0)),
        scratch_shapes=[
            pltpu.VMEM((blocks * CAP, 2 * width), jnp.bfloat16),
            pltpu.VMEM((blocks // 2, LANES), jnp.int32),
        ],
        cost_estimate=pl.CostEstimate(
            flops=4 * keys_dev * blocks * CAP * width,
            bytes_accessed=4 * keys_dev * width,
            transcendentals=0,
        ),
        compiler_params=pltpu.CompilerParams(dimension_semantics=("arbitrary",)),
        name="light",
    )(base, got)


KEYS_DEV = 4096


def per_device(values, key_ids, heavy_ids, block_offsets, block_counts):
    owners = lax.axis_size("own")
    pairs = lax.axis_size("rep")
    own_index = lax.axis_index("own")
    events, width = values.shape
    keys2d = key_ids.reshape(events // LANES, LANES)
    payload = pack(values, keys2d, block_offsets, block_counts, owners)
    heavy_wide = jnp.broadcast_to(heavy_ids[:, None], (heavy_ids.shape[0], LANES))
    got, heavy_sums = exchange(payload, values, keys2d, heavy_wide, pairs, owners)
    base = (own_index * KEYS_DEV).astype(jnp.int32).reshape(1)
    light_sums = light_totals(got, base, KEYS_DEV)
    return (light_sums, heavy_sums)


def solution(mesh):
    placed = (
        P(("rep", "own"), None),
        P(("rep", "own")),
        P(),
        P(("rep", "own"), None),
        P(("rep", "own"), None),
    )
    return jax.shard_map(
        per_device,
        mesh=mesh,
        in_specs=placed,
        out_specs=(P("own", None), P("own", None)),
        check_vma=False,
    )
```

```python
import functools
import math

import jax
import jax.numpy as jnp
from jax import lax
from jax.experimental import pallas as pl
from jax.experimental.pallas import tpu as pltpu
from jax.sharding import PartitionSpec as P

CAP = 64
LANES = 128
MESH = pl.DeviceIdType.MESH


def split_bf16(rows):
    high = rows.astype(jnp.bfloat16)
    low = (rows - high.astype(jnp.float32)).astype(jnp.bfloat16)
    return jnp.concatenate([high, low], axis=1)


def pack_kernel(owners, events, offs, cnts, vals, keys, out, stage, sems):
    def start_of(o):
        return jnp.minimum(offs[0, o], events - CAP)

    def base_of(o):
        return pl.multiple_of(jnp.minimum((start_of(o) // 8) * 8, events - CAP - 8), 8)

    def copy_of(o):
        return pltpu.make_async_copy(
            vals.at[pl.ds(base_of(o), CAP + 8)], stage.at[o], sems.at[o]
        )

    @pl.loop(0, owners)
    def _(o):
        copy_of(o).start()

    lane = lax.broadcasted_iota(jnp.int32, (1, LANES), 1)
    last_row = events // LANES - 1

    @pl.loop(0, owners)
    def _(o):
        copy_of(o).wait()

    def fill(o):
        base = base_of(o)
        start = start_of(o)
        skip = offs[0, o] - start
        out[o, 0:CAP, :] = stage[o, pl.ds(start - base, CAP), :]
        row = start // LANES
        shift = start % LANES
        back = (LANES - shift) % LANES
        first = pltpu.roll(keys[pl.ds(row, 1), :], back, 1)
        second = pltpu.roll(keys[pl.ds(jnp.minimum(row + 1, last_row), 1), :], back, 1)
        joined = jnp.where(lane < LANES - shift, first, second)
        valid = (lane >= skip) & (lane < skip + cnts[0, o]) & (lane < CAP)
        block = jnp.where(valid, joined, -1)
        twice = jnp.where(lane < CAP, block, pltpu.roll(block, CAP, 1))
        out[o, CAP : CAP + 8, :] = jnp.broadcast_to(twice, (8, LANES)).astype(jnp.float32)

    unroll = math.gcd(owners, 8)

    @pl.loop(0, owners // unroll)
    def _(g):
        for u in range(unroll):
            fill(g * unroll + u)


def pack(values, keys2d, offsets, counts, owners):
    events, width = values.shape
    smem = pl.BlockSpec(memory_space=pltpu.SMEM)
    vmem = pl.BlockSpec(memory_space=pltpu.VMEM)
    return pl.pallas_call(
        functools.partial(pack_kernel, owners, events),
        out_shape=jax.ShapeDtypeStruct((owners, CAP + 8, width), jnp.float32),
        in_specs=[smem, smem, pl.BlockSpec(memory_space=pl.ANY), vmem],
        out_specs=vmem,
        scratch_shapes=[
            pltpu.VMEM((owners, CAP + 8, width), jnp.float32),
            pltpu.SemaphoreType.DMA((owners,)),
        ],
        name="pack",
    )(offsets, counts, values, keys2d)


def exchange_kernel(
    pairs, owners, step_k, payload, vals, keys, heavy, got, sums_out,
    staged, rhs, part, quad, mine, landed, final,
    vs, ls, lr, fs, fr, qs, qr, ts, tr, es, er,
):
    r = lax.axis_index("rep")
    own = lax.axis_index("own")
    core = lax.rem(own, 2)
    chip = lax.div(own, 2)
    chips = owners // 2
    events, width = vals.shape
    steps = events // step_k
    chunk = heavy.shape[0] // chips
    rows_owner = chunk // 2
    half = rows_owner // pairs
    members = 2 * pairs

    def value_copy(s):
        at = pl.ds(pl.multiple_of(s * step_k, step_k), step_k)
        return pltpu.make_async_copy(vals.at[at], staged.at[at], vs.at[s])

    for s in range(steps):
        value_copy(s).start()

    barrier = pltpu.get_barrier_semaphore()

    @pl.loop(1, owners)
    def _(d):
        pl.semaphore_signal(
            barrier, 1, device_id=(r, lax.rem(own + d, owners)), device_id_type=MESH
        )

    for m in range(2, members):
        pl.semaphore_signal(
            barrier, 1,
            device_id=(lax.rem(r + m // 2, pairs), 2 * chip + lax.rem(core + m, 2)),
            device_id_type=MESH,
        )
    pl.semaphore_wait(barrier, owners - 1 + members - 2)

    def light(d):
        dest = lax.rem(own + d, owners)
        return pltpu.make_async_remote_copy(
            src_ref=payload.at[dest], dst_ref=got.at[r * owners + own],
            send_sem=ls.at[d], recv_sem=lr.at[d],
            device_id=(r, dest), device_id_type=MESH,
        )

    here = pltpu.make_async_copy(payload.at[own], got.at[r * owners + own], ls.at[0])
    here.start()

    @pl.loop(1, owners)
    def _(d):
        light(d).start()

    def forward(d, q):
        slot = r * owners + lax.rem(own - d + owners, owners)
        return pltpu.make_async_remote_copy(
            src_ref=got.at[slot], dst_ref=got.at[slot],
            send_sem=fs.at[q - 1, d], recv_sem=fr.at[q - 1, d],
            device_id=(lax.rem(r + q, pairs), own), device_id_type=MESH,
        )

    def gather_quad(c, m):
        peer_r = lax.rem(r + m // 2, pairs)
        peer_k = lax.rem(core + m, 2)
        return pltpu.make_async_remote_copy(
            src_ref=part.at[c, peer_r, peer_k], dst_ref=quad.at[c, m - 1],
            send_sem=qs.at[c, m - 1], recv_sem=qr.at[c, m - 1],
            device_id=(peer_r, 2 * chip + peer_k), device_id_type=MESH,
        )

    def deliver(c):
        return pltpu.make_async_remote_copy(
            src_ref=mine.at[c], dst_ref=landed.at[chip],
            send_sem=ts.at[c], recv_sem=tr.at[chip],
            device_id=(r, 2 * c + core), device_id_type=MESH,
        )

    def arrival(c):
        return pltpu.make_async_remote_copy(
            src_ref=mine.at[c], dst_ref=landed.at[c],
            send_sem=ts.at[c], recv_sem=tr.at[c],
            device_id=(r, 2 * c + core), device_id_type=MESH,
        )

    for s in range(steps):
        value_copy(s).wait()
        rhs[s * step_k : (s + 1) * step_k, :] = split_bf16(staged[s * step_k : (s + 1) * step_k, :])

    group = owners // chips
    first_forward = min(3, chips)

    def chunk_at(i):
        return lax.rem(chip + 1 + i, chips)

    @pl.loop(0, chips + 4)
    def _(i):
        @pl.when(i < chips)
        def _():
            c = chunk_at(i)
            targets = heavy[pl.ds(pl.multiple_of(c * chunk, chunk), chunk), :]

            pieces = []
            for p in range(events // LANES):
                row = keys[p : p + 1, :]
                pieces.append(jnp.where(targets == row, 1.0, 0.0).astype(jnp.bfloat16))
            onehot = jnp.concatenate(pieces, axis=1)
            acc = jnp.dot(onehot, rhs[...], preferred_element_type=jnp.float32)
            sums = acc[:, :width] + acc[:, width:]
            for k in range(2):
                for side in range(pairs):
                    begin = k * rows_owner + side * half
                    part[c, side, k] = sums[begin : begin + half]

        @pl.when((i >= 1) & (i < chips + 1))
        def _():
            c = chunk_at(i - 1)
            for m in range(1, members):
                gather_quad(c, m).start()

        @pl.when((i >= 4) & (i < chips + 4))
        def _():
            c = chunk_at(i - 4)

            @pl.when(c != chip)
            def _():
                deliver(c).start()

        @pl.when((i >= 3) & (i < chips + 3))
        def _():
            c = chunk_at(i - 3)
            total = part[c, r, core]
            for m in range(1, members):
                gather_quad(c, m).wait_recv()
                total = total + quad[c, m - 1]
            mine[c] = total

        @pl.when((i >= first_forward) & (i < first_forward + chips))
        def _():
            for g in range(group):
                d = (i - first_forward) * group + g

                @pl.when(d == 0)
                def _():
                    here.wait()

                @pl.when(d > 0)
                def _():
                    light(d).wait_recv()

                for q in range(1, pairs):
                    forward(d, q).start()

    total = mine[chip]
    for j in range(1, chips):
        c = lax.rem(chip + chips - j, chips)
        arrival(c).wait_recv()
        total = total + landed[c]
    final[r] = total

    @pl.loop(1, owners)
    def _(d):
        light(d).wait_send()

    def share(q):
        return pltpu.make_async_remote_copy(
            src_ref=final.at[r], dst_ref=final.at[r],
            send_sem=es.at[q - 1], recv_sem=er.at[q - 1],
            device_id=(lax.rem(r + q, pairs), own), device_id_type=MESH,
        )

    for q in range(1, pairs):
        share(q).start()

    @pl.loop(0, owners)
    def _(d):
        for q in range(1, pairs):
            forward(d, q).wait_recv()

    @pl.loop(0, owners)
    def _(d):
        for q in range(1, pairs):
            forward(d, q).wait_send()

    @pl.loop(0, chips)
    def _(c):
        for m in range(1, members):
            gather_quad(c, m).wait_send()

        @pl.when(c != chip)
        def _():
            deliver(c).wait_send()

    for q in range(1, pairs):
        back = lax.rem(r - q + pairs, pairs)
        pltpu.make_async_remote_copy(
            src_ref=final.at[back], dst_ref=final.at[back],
            send_sem=es.at[q - 1], recv_sem=er.at[q - 1],
            device_id=(lax.rem(r + q, pairs), own), device_id_type=MESH,
        ).wait_recv()
        share(q).wait_send()
    for side in range(pairs):
        sums_out[side * half : (side + 1) * half, :] = final[side]


def exchange(payload, values, keys2d, heavy_wide, pairs, owners):
    events, width = values.shape
    heavy = heavy_wide.shape[0]
    rows_owner = heavy // owners
    half = rows_owner // pairs
    chips = owners // 2
    step_k = 1024
    vmem = pl.BlockSpec(memory_space=pltpu.VMEM)
    dma = pltpu.SemaphoreType.DMA
    members = 2 * pairs
    return pl.pallas_call(
        functools.partial(exchange_kernel, pairs, owners, step_k),
        out_shape=(
            jax.ShapeDtypeStruct((pairs * owners, CAP + 8, width), jnp.float32),
            jax.ShapeDtypeStruct((rows_owner, width), jnp.float32),
        ),
        in_specs=[vmem, pl.BlockSpec(memory_space=pl.ANY), vmem, vmem],
        out_specs=(vmem, vmem),
        scratch_shapes=[
            pltpu.VMEM((events, width), jnp.float32),
            pltpu.VMEM((events, 2 * width), jnp.bfloat16),
            pltpu.VMEM((chips, pairs, 2, half, width), jnp.float32),
            pltpu.VMEM((chips, members - 1, half, width), jnp.float32),
            pltpu.VMEM((chips, half, width), jnp.float32),
            pltpu.VMEM((chips, half, width), jnp.float32),
            pltpu.VMEM((pairs, half, width), jnp.float32),
            dma((events // step_k,)),
            dma((owners,)),
            dma((owners,)),
            dma((pairs - 1, owners)),
            dma((pairs - 1, owners)),
            dma((chips, members - 1)),
            dma((chips, members - 1)),
            dma((chips,)),
            dma((chips,)),
            dma((pairs - 1,)),
            dma((pairs - 1,)),
        ],
        cost_estimate=pl.CostEstimate(
            flops=4 * heavy * events * width, bytes_accessed=4 * events * width, transcendentals=0
        ),
        compiler_params=pltpu.CompilerParams(
            collective_id=0, has_side_effects=True, vmem_limit_bytes=50 * 1024 * 1024
        ),
        name="exchange",
    )(payload, values, keys2d, heavy_wide)


def light_kernel(base_ref, got, out, rhs, rows):
    blocks = got.shape[0]
    width = got.shape[2]

    @pl.when(pl.program_id(0) == 0)
    def _():
        lane = lax.broadcasted_iota(jnp.int32, (1, LANES), 1)
        base = base_ref[0]

        def stage(b):
            even = got[2 * b]
            odd = got[2 * b + 1]
            pair = jnp.concatenate([even[:CAP], odd[:CAP]], axis=0)
            rhs[pl.ds(pl.multiple_of(b * 2 * CAP, 2 * CAP), 2 * CAP), :] = split_bf16(pair)
            key = jnp.where(lane < CAP, even[CAP : CAP + 1], odd[CAP : CAP + 1])
            rows[pl.ds(b, 1), :] = key.astype(jnp.int32) - base

        unroll = math.gcd(blocks // 2, 4)

        @pl.loop(0, blocks // 2 // unroll)
        def _(g):
            for u in range(unroll):
                stage(g * unroll + u)

    tile = out.shape[0]
    mine = lax.broadcasted_iota(jnp.int32, (tile, LANES), 0) + pl.program_id(0) * tile
    pieces = []
    for c in range(blocks // 2):
        row = rows[c : c + 1, :]
        pieces.append(jnp.where(mine == row, 1.0, 0.0).astype(jnp.bfloat16))
    onehot = jnp.concatenate(pieces, axis=1)
    acc = jnp.dot(onehot, rhs[...], preferred_element_type=jnp.float32)
    out[...] = acc[:, :width] + acc[:, width:]


def light_totals(got, base, keys_dev):
    blocks, unused, width = got.shape
    tile = math.gcd(keys_dev, 512)
    return pl.pallas_call(
        light_kernel,
        out_shape=jax.ShapeDtypeStruct((keys_dev, width), jnp.float32),
        grid=(keys_dev // tile,),
        in_specs=[
            pl.BlockSpec(memory_space=pltpu.SMEM),
            pl.BlockSpec(got.shape, lambda i: (0, 0, 0), pipeline_mode=pl.Buffered(1)),
        ],
        out_specs=pl.BlockSpec((tile, width), lambda i: (i, 0)),
        scratch_shapes=[
            pltpu.VMEM((blocks * CAP, 2 * width), jnp.bfloat16),
            pltpu.VMEM((blocks // 2, LANES), jnp.int32),
        ],
        cost_estimate=pl.CostEstimate(
            flops=4 * keys_dev * blocks * CAP * width,
            bytes_accessed=4 * keys_dev * width,
            transcendentals=0,
        ),
        compiler_params=pltpu.CompilerParams(dimension_semantics=("arbitrary",)),
        name="light",
    )(base, got)


KEYS_DEV = 4096


def per_device(values, key_ids, heavy_ids, block_offsets, block_counts):
    owners = lax.axis_size("own")
    pairs = lax.axis_size("rep")
    own_index = lax.axis_index("own")
    events, width = values.shape
    keys2d = key_ids.reshape(events // LANES, LANES)
    payload = pack(values, keys2d, block_offsets, block_counts, owners)
    heavy_wide = jnp.broadcast_to(heavy_ids[:, None], (heavy_ids.shape[0], LANES))
    got, heavy_sums = exchange(payload, values, keys2d, heavy_wide, pairs, owners)
    base = (own_index * KEYS_DEV).astype(jnp.int32).reshape(1)
    light_sums = light_totals(got, base, KEYS_DEV)
    return (light_sums, heavy_sums)


def solution(mesh):
    placed = (
        P(("rep", "own"), None),
        P(("rep", "own")),
        P(),
        P(("rep", "own"), None),
        P(("rep", "own"), None),
    )
    return jax.shard_map(
        per_device,
        mesh=mesh,
        in_specs=placed,
        out_specs=(P("own", None), P("own", None)),
        check_vma=False,
    )
```
